8 devices in a mesh: dp: 2 (over z, y), tp: 4 (over x, core).
Axes of the slice: x: 2, y: 2, z: 1, core: 2. Of those that a mesh axis runs over, the one named last changes fastest.
Arguments:
- x: bfloat16 [32, 8, 1280], P('dp'), parts along dimension 0
- w_in: bfloat16 [1280, 4, 2560], P(None, None, 'tp')
- w_deep: bfloat16 [3, 640, 4, 2560], P(None, None, None, 'tp')
- w_rec: bfloat16 [4, 640, 4, 2560], P(None, None, None, 'tp')
- bias: float32 [4, 4, 2560], P(None, None, 'tp')
- w_proj: bfloat16 [4, 2560, 640], P(None, 'tp')
- r_init: bfloat16 [4, 32, 640], P(None, 'dp', 'tp'), parts along dimension 1
- c_init: float32 [4, 32, 2560], P(None, 'dp', 'tp'), parts along dimension 1
Outputs:
- output 1: bfloat16 [32, 8, 640], P('dp', None, 'tp'), parts along dimension 0
- output 2: bfloat16 [4, 32, 640], P(None, 'dp', 'tp'), parts along dimension 1
- output 3: float32 [4, 32, 2560], P(None, 'dp', 'tp'), parts along dimension 1
There are 2 independent parts. The reference program is written for one: setup_inputs(seed, part) draws one part's arguments, and reference() takes and returns one part's arrays. A program takes and returns all parts, laid end to end along the dimension named above; an argument that names none is the same for every part.
All inputs are finite; a program needn't handle non-finite values.
Results may differ from the reference program's by a relative error of at most 0.00819144.
Values are sent between devices in bfloat16 or wider.
A program may use at most 1 GiB of HBM per device.

```python
import jax
import jax.numpy as jnp
from jax import lax

BATCH_SIZE = 16
TIME_STEPS = 8
NUM_LAYERS = 4
INPUT_DIM = 1280
HIDDEN_DIM = 2560
PROJ_DIM = HIDDEN_DIM // 4


def setup_inputs(seed: int = 0, part: int = 0) -> dict:
    key = jax.random.key(seed)
    part_key = jax.random.fold_in(key, part)
    keys = jax.random.split(key, 6)
    part_keys = jax.random.split(part_key, 3)
    w_in = jax.random.normal(keys[0], (INPUT_DIM, 4, HIDDEN_DIM), jnp.float32) * INPUT_DIM ** -0.5
    w_deep = jax.random.normal(keys[1], (NUM_LAYERS - 1, PROJ_DIM, 4, HIDDEN_DIM), jnp.float32) * PROJ_DIM ** -0.5
    w_rec = jax.random.normal(keys[2], (NUM_LAYERS, PROJ_DIM, 4, HIDDEN_DIM), jnp.float32) * PROJ_DIM ** -0.5
    forget_mask = (jnp.arange(4) == 1).astype(jnp.float32)[:, None]
    forget_shift = jax.random.uniform(keys[3], (NUM_LAYERS, 1, HIDDEN_DIM), jnp.float32, 0.5, 2.0)
    bias = 0.3 * jax.random.normal(keys[4], (NUM_LAYERS, 4, HIDDEN_DIM), jnp.float32) + forget_shift * forget_mask
    w_proj = jax.random.normal(keys[5], (NUM_LAYERS, HIDDEN_DIM, PROJ_DIM), jnp.float32) * HIDDEN_DIM ** -0.5
    x = jax.random.normal(part_keys[0], (BATCH_SIZE, TIME_STEPS, INPUT_DIM), jnp.float32)
    r_init = 0.6 * jax.random.normal(part_keys[1], (NUM_LAYERS, BATCH_SIZE, PROJ_DIM), jnp.float32)
    c_init = jax.random.normal(part_keys[2], (NUM_LAYERS, BATCH_SIZE, HIDDEN_DIM), jnp.float32)
    return {
        'x': x.astype(jnp.bfloat16),
        'w_in': w_in.astype(jnp.bfloat16),
        'w_deep': w_deep.astype(jnp.bfloat16),
        'w_rec': w_rec.astype(jnp.bfloat16),
        'bias': bias,
        'w_proj': w_proj.astype(jnp.bfloat16),
        'r_init': r_init.astype(jnp.bfloat16),
        'c_init': c_init,
    }


def run_layer(seq_in, w_inp, w_hh, bias_l, w_p, r_start, c_start):
    in_width = seq_in.shape[-1]
    w_in_flat = w_inp.reshape(in_width, 4 * HIDDEN_DIM)
    w_hh_flat = w_hh.reshape(PROJ_DIM, 4 * HIDDEN_DIM)

    def step(carry, u_step):
        r_prev, c_prev = carry
        gates = jnp.dot(u_step, w_in_flat, preferred_element_type=jnp.float32)
        gates = gates + jnp.dot(r_prev, w_hh_flat, preferred_element_type=jnp.float32)
        gates = gates.reshape(u_step.shape[0], 4, HIDDEN_DIM) + bias_l
        in_gate = jax.nn.sigmoid(gates[:, 0])
        forget_gate = jax.nn.sigmoid(gates[:, 1])
        out_gate = jax.nn.sigmoid(gates[:, 2])
        candidate = jnp.tanh(gates[:, 3])
        c_new = forget_gate * c_prev + in_gate * candidate
        h_new = (out_gate * jnp.tanh(c_new)).astype(jnp.bfloat16)
        r_new = jnp.dot(h_new, w_p, preferred_element_type=jnp.float32).astype(jnp.bfloat16)
        return (r_new, c_new), r_new

    (r_last, c_last), r_seq = lax.scan(step, (r_start, c_start), seq_in)
    return r_seq, r_last, c_last


def reference(x, w_in, w_deep, w_rec, bias, w_proj, r_init, c_init):
    seq_first = jnp.swapaxes(x, 0, 1)
    r_seq, r_first, c_first = run_layer(seq_first, w_in, w_rec[0], bias[0], w_proj[0], r_init[0], c_init[0])

    def layer_body(seq_prev, layer_args):
        w_inp, w_hh, bias_l, w_p, r_start, c_start = layer_args
        r_seq_l, r_last_l, c_last_l = run_layer(seq_prev, w_inp, w_hh, bias_l, w_p, r_start, c_start)
        return r_seq_l, (r_last_l, c_last_l)

    r_top, (r_rest, c_rest) = lax.scan(layer_body, r_seq, (w_deep, w_rec[1:], bias[1:], w_proj[1:], r_init[1:], c_init[1:]))
    y_out = jnp.swapaxes(r_top, 0, 1)
    r_last = jnp.concatenate([r_first[None], r_rest], axis=0)
    c_last = jnp.concatenate([c_first[None], c_rest], axis=0)
    return (y_out, r_last, c_last)
```

```python
import functools

import jax
import jax.numpy as jnp
from jax import lax
from jax.experimental import pallas as pl
from jax.experimental.pallas import tpu as pltpu
from jax.sharding import PartitionSpec as P

MESH = pl.DeviceIdType.MESH
F32, BF16 = jnp.float32, jnp.bfloat16
L, T, B = 4, 8, 16
KX, KR, C = 1280, 640, 640
NB = C // 128
Q = 4 * NB
KC = 64
XC = 256
NX = KX // XC


def regroup(raw, row0, dst, dst0, scr, n):
    def chunk(j, carry):
        src = pl.multiple_of(row0 + j * (KC * Q), KC * Q)
        k0 = pl.multiple_of(dst0 + j * KC, KC)
        scr[...] = raw[pl.ds(src, KC * Q), :].astype(F32)
        for q in range(Q):
            dst[pl.ds(k0, KC), q * 128:(q + 1) * 128] = scr[pl.ds(q, KC, stride=Q), :].astype(BF16)
        return carry

    lax.fori_loop(0, n, chunk, 0)


def kernel(x_hbm, win_hbm, wdeep_hbm, wrec_hbm, bias_hbm, wproj_hbm, rinit_ref, cinit_hbm,
           y_ref, rlast_ref, c_ref,
           x_v, xraw, raw, w_v, wx, wp, bias_v, gx, scr, rbuf, rcur, yfull,
           part, csum, rx1, rx2,
           ld_sem, x_sem, w_sem, wp_sem, ri_send, ri_recv, s1, r1, s2, r2):
    dp = lax.axis_index("dp")
    me = lax.axis_index("tp")
    chip, core = me // 2, me % 2
    partner = chip * 2 + 1 - core
    other = (1 - chip) * 2

    def dev(tp):
        return (dp, tp)

    def load_w(m):
        src = wrec_hbm.at[m] if m < L else wdeep_hbm.at[m - L]
        return pltpu.make_async_copy(src.reshape(KR * Q, 128), raw.at[m], w_sem.at[m])

    def load_x(j):
        return pltpu.make_async_copy(
            win_hbm.reshape(KX * Q, 128).at[pl.ds(j * XC * Q, XC * Q)],
            xraw.at[pl.ds(j * XC * Q, XC * Q)], x_sem.at[j])

    def load_p(l):
        return pltpu.make_async_copy(wproj_hbm.at[l], wp.at[l], wp_sem.at[l])

    load_w(0).start()
    ld_x = pltpu.make_async_copy(x_hbm, x_v, ld_sem.at[0])
    ld_x.start()
    for j in range(NX):
        load_x(j).start()
    ld_b = pltpu.make_async_copy(bias_hbm, bias_v, ld_sem.at[1])
    ld_c = pltpu.make_async_copy(cinit_hbm, c_ref, ld_sem.at[2])
    ld_b.start()
    ld_c.start()
    load_p(0).start()

    peers = (partner, other, other + 1)
    barrier = pltpu.get_barrier_semaphore()
    for p in peers:
        pl.semaphore_signal(barrier, inc=1, device_id=dev(p), device_id_type=MESH)
    pl.semaphore_wait(barrier, 3)

    def piece(i, p):
        return pltpu.make_async_remote_copy(
            src_ref=rinit_ref, dst_ref=rbuf.at[me], send_sem=ri_send.at[i], recv_sem=ri_recv.at[me],
            device_id=dev(p), device_id_type=MESH)

    for i, p in enumerate(peers):
        piece(i, p).start()

    load_w(0).wait()
    regroup(raw.at[0], 0, w_v.at[0], 0, scr, KR // KC)
    ld_x.wait()
    gx[...] = jnp.zeros_like(gx)

    def x_chunk(j, carry):
        pltpu.make_async_copy(
            win_hbm.reshape(KX * Q, 128).at[pl.ds(j * XC * Q, XC * Q)],
            xraw.at[pl.ds(j * XC * Q, XC * Q)], x_sem.at[j]).wait()
        regroup(xraw, j * XC * Q, wx, 0, scr, XC // KC)
        xs = x_v[:, :, pl.ds(pl.multiple_of(j * XC, XC), XC)].reshape(B * T, XC)
        d = jnp.dot(xs, wx[...], preferred_element_type=F32)
        for q in range(Q):
            gx[q] += d[:, q * 128:(q + 1) * 128]
        return carry

    lax.fori_loop(0, NX, x_chunk, 0)

    order = (1, L, 2, L + 1, 3, L + 2)
    for m in order:
        load_w(m).start()
    for l in range(1, L):
        load_p(l).start()

    for i, p in enumerate(peers):
        piece(i, p).wait_send()
        pltpu.make_async_remote_copy(
            src_ref=rinit_ref, dst_ref=rbuf.at[p], send_sem=ri_send.at[i], recv_sem=ri_recv.at[p],
            device_id=dev(p), device_id_type=MESH).wait_recv()
    rbuf[me] = rinit_ref[...]
    for l in range(L):
        rcur[l] = jnp.concatenate([rbuf[j, l].astype(F32) for j in range(4)], axis=1).astype(BF16)
    ld_b.wait()
    ld_c.wait()

    def copy1(l, par):
        return pltpu.make_async_remote_copy(
            src_ref=part.at[l], dst_ref=rx1.at[l, par], send_sem=s1.at[l], recv_sem=r1.at[l, par],
            device_id=dev(partner), device_id_type=MESH)

    def copy2(l, par, j, rows):
        half = pl.ds(pl.multiple_of(rows * 8, 8), 8)
        return pltpu.make_async_remote_copy(
            src_ref=csum.at[l, half], dst_ref=rx2.at[l, par, half], send_sem=s2.at[l, j],
            recv_sem=r2.at[l, par, rows], device_id=dev(other + j), device_id_type=MESH)

    def node(l, t):
        @pl.when(t == 0)
        def _():
            load_p(l).wait()

        g = jnp.dot(rcur[l], w_v[l], preferred_element_type=F32)
        if l == 0:
            g = g + jnp.concatenate([gx[q, pl.ds(t, B, stride=T), :] for q in range(Q)], axis=1)
        else:
            g = g + jnp.dot(rcur[l - 1], w_v[L + l - 1], preferred_element_type=F32)
        h = []
        for cb in range(NB):
            cols = slice(cb * 128, (cb + 1) * 128)
            gate = [g[:, (cb * 4 + k) * 128:(cb * 4 + k + 1) * 128] + bias_v[l, k:k + 1, cols] for k in range(4)]
            c_new = jax.nn.sigmoid(gate[1]) * c_ref[l, :, cols] + jax.nn.sigmoid(gate[0]) * jnp.tanh(gate[3])
            c_ref[l, :, cols] = c_new
            h.append((jax.nn.sigmoid(gate[2]) * jnp.tanh(c_new)).astype(BF16))
        part[l] = jnp.dot(jnp.concatenate(h, axis=1), wp[l], preferred_element_type=F32)
        copy1(l, t % 2).start()

    def middle(l, t):
        par = t % 2
        copy1(l, par).wait_recv()
        csum[l] = part[l] + rx1[l, par]
        for j in range(2):
            copy2(l, par, j, core).start()

    def final(l, t):
        par = t % 2
        for rows in range(2):
            copy2(l, par, 0, rows).wait_recv()
        copy1(l, par).wait_send()
        for j in range(2):
            copy2(l, par, j, core).wait_send()
        r = (csum[l] + rx2[l, par]).astype(BF16)
        rcur[l] = r
        if l == L - 1:
            for q in range(KR // 128):
                yfull[q, pl.ds(t, B, stride=T), :] = r[:, q * 128:(q + 1) * 128].astype(F32)

    def regroup_w(m):
        load_w(m).wait()
        regroup(raw.at[m], 0, w_v.at[m], 0, scr, KR // KC)

    def round_(s, carry):
        def active(l, back):
            t = s - back - l
            return jnp.logical_and(t >= 0, t < T)

        for l in range(L):
            @pl.when(active(l, 1))
            def _():
                final(l, s - 1 - l)

            @pl.when(active(l, 0))
            def _():
                node(l, s - l)

            if l > 0:
                @pl.when(active(l - 1, 0))
                def _():
                    if l < L:
                        @pl.when(s == l - 1)
                        def _():
                            regroup_w(l)
                    middle(l - 1, s - l + 1)
            if l > 0:
                @pl.when(s == l - 1)
                def _():
                    regroup_w(L + l - 1)

        @pl.when(active(L - 1, 0))
        def _():
            middle(L - 1, s - L + 1)
        return carry

    lax.fori_loop(0, T + L, round_, 0)

    for j in range(4):
        @pl.when(me == j)
        def _():
            cols = slice(j * 160, (j + 1) * 160)
            y = jnp.concatenate([yfull[q] for q in range(KR // 128)], axis=1)[:, cols]
            y_ref[...] = y.reshape(B, T, 160).astype(BF16)
            rlast_ref[...] = rcur[:, :, cols]


def solution(mesh):
    def local(x, w_in, w_deep, w_rec, bias, w_proj, r_init, c_init):
        def split(w):
            w = w.reshape(w.shape[:-1] + (NB, 128))
            return jnp.swapaxes(w, -3, -2)

        any_ = pl.BlockSpec(memory_space=pl.ANY)
        vmem = pl.BlockSpec(memory_space=pltpu.VMEM)
        dma = pltpu.SemaphoreType.DMA
        return pl.pallas_call(
            kernel,
            out_shape=(jax.ShapeDtypeStruct((B, T, 160), BF16),
                       jax.ShapeDtypeStruct((L, B, 160), BF16),
                       jax.ShapeDtypeStruct((L, B, C), F32)),
            in_specs=[any_] * 6 + [vmem, any_],
            out_specs=(vmem, vmem, vmem),
            scratch_shapes=[
                pltpu.VMEM((B, T, KX), BF16),
                pltpu.VMEM((KX * Q, 128), BF16),
                pltpu.VMEM((2 * L - 1, KR * Q, 128), BF16),
                pltpu.VMEM((2 * L - 1, KR, 4 * C), BF16),
                pltpu.VMEM((XC, 4 * C), BF16),
                pltpu.VMEM((L, C, KR), BF16),
                pltpu.VMEM((L, 4, C), F32),
                pltpu.VMEM((Q, B * T, 128), F32),
                pltpu.VMEM((KC * Q, 128), F32),
                pltpu.VMEM((4, L, B, 160), BF16),
                pltpu.VMEM((L, B, KR), BF16),
                pltpu.VMEM((KR // 128, B * T, 128), F32),
                pltpu.VMEM((L, B, KR), F32),
                pltpu.VMEM((L, B, KR), F32),
                pltpu.VMEM((L, 2, B, KR), F32),
                pltpu.VMEM((L, 2, B, KR), F32),
                dma((3,)), dma((NX,)), dma((2 * L - 1,)), dma((L,)),
                dma((3,)), dma((4,)), dma((L,)), dma((L, 2)), dma((L, 2)), dma((L, 2, 2)),
            ],
            compiler_params=pltpu.CompilerParams(
                collective_id=0, has_side_effects=True, vmem_limit_bytes=66_000_000),
        )(x, split(w_in), split(w_deep), split(w_rec), bias, w_proj, r_init, c_init)

    specs_in = (P('dp', None, None), P(None, None, 'tp'), P(None, None, None, 'tp'), P(None, None, None, 'tp'),
                P(None, None, 'tp'), P(None, 'tp', None), P(None, 'dp', 'tp'), P(None, 'dp', 'tp'))
    specs_out = (P('dp', None, 'tp'), P(None, 'dp', 'tp'), P(None, 'dp', 'tp'))
    return jax.shard_map(local, mesh=mesh, in_specs=specs_in, out_specs=specs_out, check_vma=False)
```
